8 devices in a mesh: dp: 1 (over z), tp: 8 (over y, x, core).
Axes of the slice: x: 2, y: 2, z: 1, core: 2. Of those that a mesh axis runs over, the one named last changes fastest.
Arguments:
- hidden: bfloat16 [4096, 4096], P(('dp', 'tp'))
- ln_gain: float32 [4096], replicated
- ln_bias: float32 [4096], replicated
- out_embed: bfloat16 [32768, 4096], P('tp')
- vocab_valid: int32 [32768], P('tp')
- targets: int32 [4096], P(('dp', 'tp'))
- loss_mask: int32 [4096], P(('dp', 'tp'))
Outputs:
- output 1: float32 [4096], P(('dp', 'tp'))
- output 2: float32 [1], P('dp')
- output 3: bfloat16 [4096, 4096], P(('dp', 'tp'))
- output 4: float32 [32768, 4096], P(('dp', 'tp'))
- output 5: float32 [4096], P('dp')
- output 6: float32 [4096], P('dp')
All inputs are finite; a program needn't handle non-finite values.
Results may differ from the reference program's by a relative error of at most 0.001.
Values are sent between devices in bfloat16 or wider.
A program may use at most 1 GiB of HBM per device.

```python
import jax
import jax.numpy as jnp
from jax import lax

MODEL_DIM = 4096
VOCAB_REAL = 32768
VOCAB_PAD = 32768
SEQ_LEN = 4096
TOK_BLOCK = 512
BLOCK_COUNT = SEQ_LEN // TOK_BLOCK
SOFT_CAP = 30.0
Z_COEF = 1e-4
LN_EPS = 1e-5


def layer_norm(h_float, ln_gain, ln_bias):
    mean_val = jnp.mean(h_float, axis=-1, keepdims=True)
    centered = h_float - mean_val
    var_val = jnp.mean(centered * centered, axis=-1, keepdims=True)
    return centered * lax.rsqrt(var_val + LN_EPS) * ln_gain + ln_bias


def draw_layout(shared_key, part_key):
    col_idx = jnp.arange(VOCAB_PAD)
    coin_draw = jax.random.randint(shared_key, (VOCAB_PAD,), 0, 8)
    dropped = (col_idx % 2 == 0) & (coin_draw == 0) & (col_idx < VOCAB_REAL - 1)
    vocab_valid = ((col_idx < VOCAB_REAL) & jnp.logical_not(dropped)).astype(jnp.int32)
    key_tgt, key_pre, key_post, key_hole = jax.random.split(part_key, 4)
    raw_tgt = jax.random.randint(key_tgt, (SEQ_LEN,), 0, VOCAB_REAL)
    targets = raw_tgt + 1 - vocab_valid[raw_tgt]
    positions = jnp.arange(SEQ_LEN)
    prefix_len = jax.random.randint(key_pre, (), 0, SEQ_LEN // 4 + 1)
    suffix_len = jax.random.randint(key_post, (), 0, SEQ_LEN // 4 + 1)
    hole_draw = jax.random.randint(key_hole, (SEQ_LEN,), 0, 8)
    keep_tok = (positions >= prefix_len) & (positions < SEQ_LEN - suffix_len) & (hole_draw != 0)
    keep_tok = keep_tok | (positions == SEQ_LEN // 2)
    return vocab_valid, targets.astype(jnp.int32), keep_tok.astype(jnp.int32)


def setup_inputs(seed: int = 0, part: int = 0) -> dict:
    shared_key = jax.random.key(seed)
    part_key = jax.random.fold_in(jax.random.key(seed + 1), part)
    key_gain, key_bias, key_embed, key_valid = jax.random.split(shared_key, 4)
    key_hidden, key_layout = jax.random.split(part_key, 2)
    hidden = 1.5 * jax.random.normal(key_hidden, (SEQ_LEN, MODEL_DIM), jnp.float32)
    ln_gain = 1.0 + 0.3 * jax.random.normal(key_gain, (MODEL_DIM,), jnp.float32)
    ln_bias = 0.3 * jax.random.normal(key_bias, (MODEL_DIM,), jnp.float32)
    out_embed = (3.0 * MODEL_DIM ** -0.5) * jax.random.normal(key_embed, (VOCAB_PAD, MODEL_DIM), jnp.float32)
    vocab_valid, targets, loss_mask = draw_layout(key_valid, key_layout)
    return {"hidden": hidden.astype(jnp.bfloat16), "ln_gain": ln_gain, "ln_bias": ln_bias, "out_embed": out_embed.astype(jnp.bfloat16), "vocab_valid": vocab_valid, "targets": targets, "loss_mask": loss_mask}


def reference(hidden, ln_gain, ln_bias, out_embed, vocab_valid, targets, loss_mask):
    normed, ln_back = jax.vjp(layer_norm, hidden.astype(jnp.float32), ln_gain, ln_bias)
    x_all = normed.astype(jnp.bfloat16)
    mask_f = loss_mask.astype(jnp.float32)
    tok_count = jnp.sum(mask_f)
    col_ok = (vocab_valid != 0)[None, :]
    col_ids = jnp.arange(VOCAB_PAD)[None, :]

    def block_step(embed_grad, blk_data):
        x_blk, tgt_blk, mask_blk = blk_data
        logits = jnp.dot(x_blk, out_embed.T, preferred_element_type=jnp.float32)
        tanh_val = jnp.tanh(logits / SOFT_CAP)
        capped = SOFT_CAP * tanh_val
        masked = jnp.where(col_ok, capped, -SOFT_CAP)
        row_max = jnp.max(masked, axis=1, keepdims=True)
        exp_vals = jnp.where(col_ok, jnp.exp(masked - row_max), 0.0)
        sum_exp = jnp.sum(exp_vals, axis=1, keepdims=True)
        lse = row_max[:, 0] + jnp.log(sum_exp[:, 0])
        is_target = tgt_blk[:, None] == col_ids
        tgt_logit = jnp.sum(jnp.where(is_target, capped, 0.0), axis=1)
        tok_loss = (lse - tgt_logit + Z_COEF * lse * lse) * mask_blk
        tok_coef = mask_blk / tok_count
        d_capped = ((1.0 + 2.0 * Z_COEF * lse) * tok_coef)[:, None] * (exp_vals / sum_exp) - jnp.where(is_target, tok_coef[:, None], 0.0)
        d_logits = (d_capped * (1.0 - tanh_val * tanh_val)).astype(jnp.bfloat16)
        new_grad = embed_grad + jnp.dot(d_logits.T, x_blk, preferred_element_type=jnp.float32)
        d_normed = jnp.dot(d_logits, out_embed, preferred_element_type=jnp.float32)
        return new_grad, (tok_loss, d_normed)

    init_grad = jnp.zeros((VOCAB_PAD, MODEL_DIM), jnp.float32)
    blk_inputs = (x_all.reshape(BLOCK_COUNT, TOK_BLOCK, MODEL_DIM), targets.reshape(BLOCK_COUNT, TOK_BLOCK), mask_f.reshape(BLOCK_COUNT, TOK_BLOCK))
    d_embed, (tok_loss, d_normed) = lax.scan(block_step, init_grad, blk_inputs)
    tok_loss = tok_loss.reshape(SEQ_LEN)
    d_normed = d_normed.reshape(SEQ_LEN, MODEL_DIM)
    mean_loss = jnp.sum(tok_loss) / tok_count
    d_hidden, d_gain, d_bias = ln_back(d_normed)
    return tok_loss, mean_loss.reshape(1), d_hidden.astype(jnp.bfloat16), d_embed, d_gain, d_bias
```

```python
import jax
import jax.numpy as jnp
from jax import lax
from jax.experimental import pallas as pl
from jax.experimental.pallas import tpu as pltpu
from jax.sharding import PartitionSpec as P


MESH = pl.DeviceIdType.MESH
SOFT_CAP = 30.0
Z_COEF = 1e-4
LN_EPS = 1e-5
PIECE = 128
TV = 1024


def batch_rows(b):
    k1 = b - 4
    k2 = b - 12
    row_a = jnp.where(b < 4, 256 * b, jnp.where(b < 12, (2 + k1 % 2) * 512 + (k1 // 2) * PIECE, (6 + k2 % 2) * 512 + (k2 // 2) * PIECE))
    row_b = jnp.where(b < 4, 256 * b + PIECE, jnp.where(b < 12, (4 + k1 % 2) * 512 + (k1 // 2) * PIECE, (6 + k2 % 2) * 512 + (2 + k2 // 2) * PIECE))
    return row_a, row_b


def static_rows(b):
    if b < 4:
        return 256 * b, 256 * b + PIECE
    if b < 12:
        k = b - 4
        return (2 + k % 2) * 512 + (k // 2) * PIECE, (4 + k % 2) * 512 + (k // 2) * PIECE
    k = b - 12
    return (6 + k % 2) * 512 + (k // 2) * PIECE, (6 + k % 2) * 512 + (2 + k // 2) * PIECE


def logits_kernel(x_own, embed, meta_own, valid, xall, grad, stats, meta, e_vmem, xbuf, acc0, acc1, out, part_s, part_t, mine, others, e_sem, x_sem, g_sem, own_sem, send_sem, recv_sem, meta_send, meta_recv, stat_send, stat_recv):
    me = lax.axis_index("tp")
    tiles = e_vmem.shape[0] // TV
    n_batch = xall.shape[0] // 256

    def peer(bit):
        return {"tp": me ^ bit}

    def fwd(src, row, bit, idx):
        return pltpu.make_async_remote_copy(src_ref=src, dst_ref=xall.at[pl.ds(row, PIECE)], send_sem=send_sem.at[idx], recv_sem=recv_sem.at[idx], device_id=peer(bit), device_id_type=MESH)

    copies = {}
    for p in range(4):
        own = x_own.at[pl.ds(p * PIECE, PIECE)]
        for r in (1, 2, 4):
            copies[r, p] = fwd(own, r * 512 + p * PIECE, r, r * 4 + p)
        copies[3, p] = fwd(xall.at[pl.ds(2 * 512 + p * PIECE, PIECE)], 3 * 512 + p * PIECE, 1, 12 + p)
        copies[5, p] = fwd(xall.at[pl.ds(4 * 512 + p * PIECE, PIECE)], 5 * 512 + p * PIECE, 1, 20 + p)
        via = (2, 4) if p < 2 else (4, 2)
        copies[6, p] = fwd(xall.at[pl.ds(via[0] * 512 + p * PIECE, PIECE)], 6 * 512 + p * PIECE, via[1], 24 + p)
        copies[7, p] = fwd(xall.at[pl.ds(6 * 512 + p * PIECE, PIECE)], 7 * 512 + p * PIECE, 1, 28 + p)

    e_copies = [pltpu.make_async_copy(embed.at[pl.ds(t * TV, TV)], e_vmem.at[pl.ds(t * TV, TV)], e_sem.at[t]) for t in range(tiles)]
    own_loads = [pltpu.make_async_copy(x_own.at[pl.ds(k * 256, 256)], xbuf.at[k], x_sem.at[2 * k]) for k in range(2)]
    own_stores = [pltpu.make_async_copy(xbuf.at[k], xall.at[pl.ds(k * 256, 256)], own_sem.at[k]) for k in range(2)]
    own_loads[0].start()
    e_copies[0].start()
    own_loads[1].start()
    for t in range(1, tiles):
        e_copies[t].start()

    barrier = pltpu.get_barrier_semaphore()
    for bit in range(1, 8):
        pl.semaphore_signal(barrier, inc=1, device_id=peer(bit), device_id_type=MESH)
    pl.semaphore_wait(barrier, 7)
    for p in range(4):
        for r in (2, 4):
            copies[r, p].start()
    for p in range(4):
        copies[1, p].start()
    meta_copies = [pltpu.make_async_remote_copy(src_ref=meta_own, dst_ref=meta.at[bit], send_sem=meta_send.at[bit], recv_sem=meta_recv.at[bit], device_id=peer(bit), device_id_type=MESH) for bit in range(1, 8)]
    for c in meta_copies:
        c.start()
    meta[0] = meta_own[...]
    own_loads[0].wait()
    own_stores[0].start()
    own_loads[1].wait()
    own_stores[1].start()

    def arrive(batch):
        if batch in (2, 3):
            for p in range(2):
                copies[1, 2 * (batch - 2) + p].wait_recv()
        elif 4 <= batch < 12 and batch % 2 == 0:
            p = (batch - 4) // 2
            copies[2, p].wait_recv()
            copies[3, p].start()
            if p < 2:
                copies[6, p].start()
            copies[4, p].wait_recv()
            copies[5, p].start()
            if p >= 2:
                copies[6, p].start()
        elif 4 <= batch < 12:
            p = (batch - 4) // 2
            copies[3, p].wait_recv()
            copies[5, p].wait_recv()
        elif batch % 2 == 0:
            h = (batch - 12) // 2
            for p in (h, 2 + h):
                copies[6, p].wait_recv()
                copies[7, p].start()
        else:
            h = (batch - 12) // 2
            for p in (h, 2 + h):
                copies[7, p].wait_recv()
        if batch == 2:
            for c in meta_copies:
                c.wait_recv()

    def loads(b):
        rows = batch_rows(b)
        slot = b % 2
        return [pltpu.make_async_copy(xall.at[pl.ds(pl.multiple_of(rows[k], PIECE), PIECE)], xbuf.at[slot, pl.ds(k * PIECE, PIECE)], x_sem.at[2 * slot + k]) for k in range(2)]

    row_iota = lax.broadcasted_iota(jnp.int32, (TV, 256), 0)

    def store(b, j):
        rows = batch_rows(b)
        slot = (b + 2) % 2 * tiles + j
        return [pltpu.make_async_copy(out.at[slot, k], grad.at[pl.ds(j * TV, TV), pl.ds(pl.multiple_of(rows[k], PIECE), PIECE)], g_sem.at[2 * slot + k]) for k in range(2)]

    def epilogue(b, j, acc):
        rows = batch_rows(b)
        tgt = jnp.concatenate([meta[rows[k] // 512, pl.ds((rows[k] // PIECE) % 4, 1), :] for k in range(2)], axis=1)
        ok = valid[j * TV:(j + 1) * TV, :]
        t = jnp.tanh(acc[...] * (1.0 / SOFT_CAP))
        e = jnp.exp(t * SOFT_CAP) * ok
        hit = jnp.where(row_iota == tgt - (me * (tiles * TV) + j * TV), t, 0.0)
        g = e * (1.0 - t * t)
        slot = (b + 2) % 2 * tiles + j
        for k in range(2):
            out[slot, k] = g[:, k * PIECE:(k + 1) * PIECE]
        part_s[b * tiles + j] = jnp.sum(e.reshape(TV // 8, 8, 256), axis=0)
        part_t[b * tiles + j] = jnp.sum(hit.reshape(TV // 8, 8, 256), axis=0)

    def dot(b, j, acc):
        acc[...] = lax.dot_general(e_vmem[j * TV:(j + 1) * TV, :], xbuf[b % 2], (((1,), (1,)), ((), ())), preferred_element_type=jnp.float32)

    def body(b, carry):
        before = jnp.maximum(b - 1, 0)

        @pl.when(b == 0)
        def _():
            e_copies[0].wait()
            e_copies[1].wait()

        @pl.when(b >= 2)
        def _():
            for c in loads(b):
                c.wait()

        @pl.when(b >= 3)
        def _():
            for c in store(b - 3, 3):
                c.wait()

        @pl.when(b >= 2)
        def _():
            for j in range(tiles - 1):
                for c in store(b - 2, j):
                    c.wait()

        dot(b, 0, acc0)
        epilogue(before, 3, acc1)
        dot(b, 1, acc1)
        epilogue(b, 0, acc0)

        @pl.when(b == 0)
        def _():
            e_copies[2].wait()
            e_copies[3].wait()
            own_stores[1].wait()

        @pl.when(b == 1)
        def _():
            own_stores[0].wait()

        for nb in range(2, n_batch):
            @pl.when(b == nb - 1)
            def _():
                arrive(nb)

        @pl.when((b >= 1) & (b < n_batch - 1))
        def _():
            for c in loads(b + 1):
                c.start()

        @pl.when(b >= 1)
        def _():
            for c in store(b - 1, 3):
                c.start()

        for c in store(b, 0):
            c.start()
        dot(b, 2, acc0)
        epilogue(b, 1, acc1)
        dot(b, 3, acc1)
        epilogue(b, 2, acc0)
        for j in (1, 2):
            for c in store(b, j):
                c.start()
        return carry

    lax.fori_loop(0, n_batch, body, 0)
    last = n_batch - 1
    for c in store(last - 2, 3):
        c.wait()
    epilogue(last, 3, acc1)
    for c in store(last, 3):
        c.start()
    for b in range(n_batch):
        s_sum = jnp.sum(part_s[b * tiles:(b + 1) * tiles], axis=(0, 1))
        t_sum = jnp.sum(part_t[b * tiles:(b + 1) * tiles], axis=(0, 1))
        for k, row in enumerate(static_rows(b)):
            r, p = row // 512, (row // PIECE) % 4
            mine[r, p:p + 1, :] = s_sum[None, k * PIECE:(k + 1) * PIECE]
            mine[r, 4 + p:5 + p, :] = t_sum[None, k * PIECE:(k + 1) * PIECE]
    for j in range(tiles - 1):
        for c in store(last - 1, j) + store(last, j):
            c.wait()
    for c in store(last - 1, 3) + store(last, 3):
        c.wait()
    stat_copies = [pltpu.make_async_remote_copy(src_ref=mine, dst_ref=others.at[bit - 1], send_sem=stat_send.at[bit], recv_sem=stat_recv.at[bit], device_id=peer(bit), device_id_type=MESH) for bit in range(1, 8)]
    for c in stat_copies:
        c.start()
    for c in meta_copies:
        c.wait_send()
    for c in copies.values():
        c.wait_send()
    for c in stat_copies:
        c.wait()
    for r in range(8):
        t = [mine[r]] + [others[bit - 1, r ^ bit] for bit in range(1, 8)]
        stats[r] = ((t[0] + t[1]) + (t[2] + t[3])) + ((t[4] + t[5]) + (t[6] + t[7]))


def gather_logits(x_own, embed, meta_own, valid):
    rows, dim = x_own.shape
    vocab = embed.shape[0]
    toks = 8 * rows
    any_spec = pl.BlockSpec(memory_space=pl.ANY)
    vmem_spec = pl.BlockSpec(memory_space=pltpu.VMEM)
    steps = toks // 256 * (vocab // TV)
    return pl.pallas_call(
        logits_kernel,
        name="gather_logits",
        out_shape=(jax.ShapeDtypeStruct((toks, dim), jnp.bfloat16), jax.ShapeDtypeStruct((vocab, toks), jnp.float32), jax.ShapeDtypeStruct((8, 8, 128), jnp.float32), jax.ShapeDtypeStruct((8, 8, 128), jnp.int32)),
        in_specs=[any_spec, any_spec, vmem_spec, vmem_spec],
        out_specs=(any_spec, any_spec, vmem_spec, vmem_spec),
        scratch_shapes=[
            pltpu.VMEM((vocab, dim), jnp.bfloat16),
            pltpu.VMEM((2, 256, dim), jnp.bfloat16),
            pltpu.VMEM((TV, 256), jnp.float32),
            pltpu.VMEM((TV, 256), jnp.float32),
            pltpu.VMEM((2 * vocab // TV, 2, TV, PIECE), jnp.float32),
            pltpu.VMEM((steps, 8, 256), jnp.float32),
            pltpu.VMEM((steps, 8, 256), jnp.float32),
            pltpu.VMEM((8, 8, 128), jnp.float32),
            pltpu.VMEM((7, 8, 8, 128), jnp.float32),
            pltpu.SemaphoreType.DMA((vocab // TV,)),
            pltpu.SemaphoreType.DMA((4,)),
            pltpu.SemaphoreType.DMA((4 * vocab // TV,)),
            pltpu.SemaphoreType.DMA((2,)),
            pltpu.SemaphoreType.DMA((32,)),
            pltpu.SemaphoreType.DMA((32,)),
            pltpu.SemaphoreType.DMA((8,)),
            pltpu.SemaphoreType.DMA((8,)),
            pltpu.SemaphoreType.DMA((8,)),
            pltpu.SemaphoreType.DMA((8,)),
        ],
        compiler_params=pltpu.CompilerParams(collective_id=0, has_side_effects=True, vmem_limit_bytes=60 * 1024 * 1024),
        cost_estimate=pl.CostEstimate(flops=2 * toks * vocab * dim, bytes_accessed=vocab * dim * 2 + toks * vocab * 4, transcendentals=2 * toks * vocab),
    )(x_own, embed, meta_own, valid)


def layer_norm(h_float, ln_gain, ln_bias):
    mean_val = jnp.mean(h_float, axis=-1, keepdims=True)
    centered = h_float - mean_val
    var_val = jnp.mean(centered * centered, axis=-1, keepdims=True)
    return centered * lax.rsqrt(var_val + LN_EPS) * ln_gain + ln_bias


def solution(mesh):
    def swap(bit, x):
        return lax.ppermute(x, "tp", [(i, i ^ bit) for i in range(8)])

    def group_step(hidden, ln_gain, ln_bias, out_embed, vocab_valid, targets, loss_mask):
        rows_loc, dim = hidden.shape
        vocab_loc = out_embed.shape[0]
        shard_idx = lax.axis_index("tp")
        normed, ln_back = jax.vjp(layer_norm, hidden.astype(jnp.float32), ln_gain, ln_bias)
        meta_own = jnp.concatenate([targets.reshape(4, PIECE), loss_mask.reshape(4, PIECE)])
        x_all, grad, stats, meta = gather_logits(normed.astype(jnp.bfloat16), out_embed, meta_own, (vocab_valid != 0).astype(jnp.float32)[:, None])
        sum_exp = stats[:, :4].reshape(8, rows_loc)
        tgt_tanh = stats[:, 4:].reshape(8, rows_loc)
        tgt_row = meta[:, :4].reshape(8 * rows_loc) - shard_idx * vocab_loc
        mask_all = meta[:, 4:].reshape(8, rows_loc).astype(jnp.float32)

        def group_sum(part):
            return ((part[0] + part[1]) + (part[2] + part[3])) + ((part[4] + part[5]) + (part[6] + part[7]))

        tok_count = group_sum(jnp.sum(mask_all, axis=1))
        lse = jnp.log(sum_exp)
        loss_all = (lse - SOFT_CAP * tgt_tanh + Z_COEF * lse * lse) * mask_all
        mean_loss = group_sum(jnp.sum(loss_all, axis=1)) / tok_count
        tok_coef = mask_all / tok_count
        prob_coef = ((1.0 + 2.0 * Z_COEF * lse) * tok_coef / sum_exp).reshape(1, 8 * rows_loc)
        tgt_coef = (tok_coef * (1.0 - tgt_tanh * tgt_tanh)).reshape(1, 8 * rows_loc)
        is_target = tgt_row[None, :] == jnp.arange(vocab_loc)[:, None]
        d_logits = (prob_coef * grad - jnp.where(is_target, tgt_coef, 0.0)).astype(jnp.bfloat16)
        d_logits = lax.optimization_barrier(d_logits)

        mid = dim // 2

        def part(d_log, r, c):
            rows = d_log[:, r * rows_loc:(r + 1) * rows_loc]
            return lax.dot_general(rows, out_embed[:, c * mid:(c + 1) * mid], (((0,), (0,)), ((), ())), preferred_element_type=jnp.float32)

        def after(d_log, *done):
            return lax.optimization_barrier((d_log, *done))

        far = [part(d_logits, 7, c) for c in range(2)]
        step, *far = after(d_logits, *far)
        pair_far = [part(step, 6, c) + swap(1, far[c]) for c in range(2)]
        step, *pair_far = after(step, *pair_far)
        to_x, to_y = swap(2, pair_far[0]), swap(4, pair_far[1])
        near = [part(step, 3, 0), part(step, 5, 1), part(step, 3, 1), part(step, 5, 0)]
        step, *near = after(step, *near)
        late = [swap(1, near[2]), swap(1, near[3])]
        early = [swap(1, near[0]), swap(1, near[1])]
        first = [part(step, 2, 0) + early[0], part(step, 4, 1) + early[1]]
        step, *first = after(step, *first)
        from_x, from_y = [swap(2, first[0]), None], [None, swap(4, first[1])]
        other = [part(step, 1, c) for c in range(2)]
        step, *other = after(step, *other)
        own = [part(step, 0, c) + swap(1, other[c]) for c in range(2)]
        step, *own = after(step, *own)
        second = [part(step, 2, 1) + late[0] + to_y, part(step, 4, 0) + late[1] + to_x]
        step, *second = after(step, *second)
        from_x[1], from_y[0] = swap(2, second[0]), swap(4, second[1])
        d_embed = lax.dot_general(step, x_all, (((1,), (0,)), ((), ())), preferred_element_type=jnp.float32)
        d_normed = jnp.concatenate([own[c] + from_x[c] + from_y[c] for c in range(2)], axis=1)
        d_hidden, gain_part, bias_part = ln_back(d_normed)
        d_both = lax.psum(jnp.stack([gain_part, bias_part]), "tp")
        tok_loss = loss_all[0]
        return tok_loss, mean_loss.reshape(1), d_hidden.astype(jnp.bfloat16), d_embed, d_both[0], d_both[1]

    row_spec = P(("dp", "tp"))
    mat_spec = P(("dp", "tp"), None)

    return jax.shard_map(group_step, mesh=mesh, in_specs=(mat_spec, P(None), P(None), P("tp", None), P("tp"), row_spec, row_spec), out_specs=(row_spec, P("dp"), mat_spec, mat_spec, P("dp"), P("dp")), check_vma=False)
```

```python
import functools

import jax
import jax.numpy as jnp
from jax import lax
from jax.experimental import pallas as pl
from jax.experimental.pallas import tpu as pltpu
from jax.sharding import PartitionSpec as P


MESH = pl.DeviceIdType.MESH
SOFT_CAP = 30.0
Z_COEF = 1e-4
LN_EPS = 1e-5
PIECE = 128
TV = 1024


def batch_rows(b):
    k1 = b - 4
    k2 = b - 12
    row_a = jnp.where(b < 4, 256 * b, jnp.where(b < 12, (2 + k1 % 2) * 512 + (k1 // 2) * PIECE, (6 + k2 % 2) * 512 + (k2 // 2) * PIECE))
    row_b = jnp.where(b < 4, 256 * b + PIECE, jnp.where(b < 12, (4 + k1 % 2) * 512 + (k1 // 2) * PIECE, (6 + k2 % 2) * 512 + (2 + k2 // 2) * PIECE))
    return row_a, row_b


def static_rows(b):
    if b < 4:
        return 256 * b, 256 * b + PIECE
    if b < 12:
        k = b - 4
        return (2 + k % 2) * 512 + (k // 2) * PIECE, (4 + k % 2) * 512 + (k // 2) * PIECE
    k = b - 12
    return (6 + k % 2) * 512 + (k // 2) * PIECE, (6 + k % 2) * 512 + (2 + k // 2) * PIECE


def logits_kernel(x_own, embed, meta_own, valid, xall, grad, stats, meta, e_vmem, xbuf, acc0, acc1, out, part_s, part_t, mine, others, e_sem, x_sem, g_sem, own_sem, send_sem, recv_sem, meta_send, meta_recv, stat_send, stat_recv):
    me = lax.axis_index("tp")
    tiles = e_vmem.shape[0] // TV
    n_batch = xall.shape[0] // 256

    def peer(bit):
        return {"tp": me ^ bit}

    def fwd(src, row, bit, idx):
        return pltpu.make_async_remote_copy(src_ref=src, dst_ref=xall.at[pl.ds(row, PIECE)], send_sem=send_sem.at[idx], recv_sem=recv_sem.at[idx], device_id=peer(bit), device_id_type=MESH)

    copies = {}
    for p in range(4):
        own = x_own.at[pl.ds(p * PIECE, PIECE)]
        for r in (1, 2, 4):
            copies[r, p] = fwd(own, r * 512 + p * PIECE, r, r * 4 + p)
        copies[3, p] = fwd(xall.at[pl.ds(2 * 512 + p * PIECE, PIECE)], 3 * 512 + p * PIECE, 1, 12 + p)
        copies[5, p] = fwd(xall.at[pl.ds(4 * 512 + p * PIECE, PIECE)], 5 * 512 + p * PIECE, 1, 20 + p)
        via = (2, 4) if p < 2 else (4, 2)
        copies[6, p] = fwd(xall.at[pl.ds(via[0] * 512 + p * PIECE, PIECE)], 6 * 512 + p * PIECE, via[1], 24 + p)
        copies[7, p] = fwd(xall.at[pl.ds(6 * 512 + p * PIECE, PIECE)], 7 * 512 + p * PIECE, 1, 28 + p)

    e_copies = [pltpu.make_async_copy(embed.at[pl.ds(t * TV, TV)], e_vmem.at[pl.ds(t * TV, TV)], e_sem.at[t]) for t in range(tiles)]
    own_loads = [pltpu.make_async_copy(x_own.at[pl.ds(k * 256, 256)], xbuf.at[k], x_sem.at[2 * k]) for k in range(2)]
    own_stores = [pltpu.make_async_copy(xbuf.at[k], xall.at[pl.ds(k * 256, 256)], own_sem.at[k]) for k in range(2)]
    own_loads[0].start()
    e_copies[0].start()
    own_loads[1].start()
    for t in range(1, tiles):
        e_copies[t].start()

    barrier = pltpu.get_barrier_semaphore()
    for bit in range(1, 8):
        pl.semaphore_signal(barrier, inc=1, device_id=peer(bit), device_id_type=MESH)
    pl.semaphore_wait(barrier, 7)
    for r in (2, 4):
        copies[r, 0].start()
    for p in range(4):
        copies[1, p].start()
    meta_copies = [pltpu.make_async_remote_copy(src_ref=meta_own, dst_ref=meta.at[bit], send_sem=meta_send.at[bit], recv_sem=meta_recv.at[bit], device_id=peer(bit), device_id_type=MESH) for bit in range(1, 8)]
    for c in meta_copies:
        c.start()
    meta[0] = meta_own[...]
    own_loads[0].wait()
    own_stores[0].start()
    own_loads[1].wait()
    own_stores[1].start()

    def arrive(batch):
        if batch in (2, 4, 6):
            for r in (2, 4):
                copies[r, batch // 2].start()
        elif batch in (8, 10):
            copies[6, batch // 2 - 4].start()
        if batch in (2, 3):
            for p in range(2):
                copies[1, 2 * (batch - 2) + p].wait_recv()
        elif 4 <= batch < 12 and batch % 2 == 0:
            p = (batch - 4) // 2
            copies[4, p].wait_recv()
            if p >= 2:
                copies[6, p].start()
            copies[5, p].start()
            copies[2, p].wait_recv()
            copies[3, p].start()
        elif 4 <= batch < 12:
            p = (batch - 4) // 2
            copies[3, p].wait_recv()
            copies[5, p].wait_recv()
        elif batch % 2 == 0:
            h = (batch - 12) // 2
            for p in (h, 2 + h):
                copies[6, p].wait_recv()
                copies[7, p].start()
        else:
            h = (batch - 12) // 2
            for p in (h, 2 + h):
                copies[7, p].wait_recv()
        if batch == 2:
            for c in meta_copies:
                c.wait_recv()

    def loads(b):
        rows = batch_rows(b)
        slot = b % 2
        return [pltpu.make_async_copy(xall.at[pl.ds(pl.multiple_of(rows[k], PIECE), PIECE)], xbuf.at[slot, pl.ds(k * PIECE, PIECE)], x_sem.at[2 * slot + k]) for k in range(2)]

    row_iota = lax.broadcasted_iota(jnp.int32, (TV, 256), 0)

    def store(b, j):
        rows = batch_rows(b)
        slot = (b + 2) % 2 * tiles + j
        return [pltpu.make_async_copy(out.at[slot, k], grad.at[pl.ds(j * TV, TV), pl.ds(pl.multiple_of(rows[k], PIECE), PIECE)], g_sem.at[2 * slot + k]) for k in range(2)]

    def epilogue(b, j, acc):
        rows = batch_rows(b)
        tgt = jnp.concatenate([meta[rows[k] // 512, pl.ds((rows[k] // PIECE) % 4, 1), :] for k in range(2)], axis=1)
        ok = valid[j * TV:(j + 1) * TV, :]
        t = jnp.tanh(acc[...] * (1.0 / SOFT_CAP))
        e = jnp.exp(t * SOFT_CAP) * ok
        hit = jnp.where(row_iota == tgt - (me * (tiles * TV) + j * TV), t, 0.0)
        g = e * (1.0 - t * t)
        slot = (b + 2) % 2 * tiles + j
        for k in range(2):
            out[slot, k] = g[:, k * PIECE:(k + 1) * PIECE]
        part_s[b * tiles + j] = jnp.sum(e.reshape(TV // 8, 8, 256), axis=0)
        part_t[b * tiles + j] = jnp.sum(hit.reshape(TV // 8, 8, 256), axis=0)

    def dot(b, j, acc):
        acc[...] = lax.dot_general(e_vmem[j * TV:(j + 1) * TV, :], xbuf[b % 2], (((1,), (1,)), ((), ())), preferred_element_type=jnp.float32)

    def body(b, carry):
        before = jnp.maximum(b - 1, 0)

        @pl.when(b == 0)
        def _():
            e_copies[0].wait()
            e_copies[1].wait()

        @pl.when(b >= 2)
        def _():
            for c in loads(b):
                c.wait()

        @pl.when(b >= 3)
        def _():
            for c in store(b - 3, 3):
                c.wait()

        @pl.when(b >= 2)
        def _():
            for j in range(tiles - 1):
                for c in store(b - 2, j):
                    c.wait()

        dot(b, 0, acc0)
        epilogue(before, 3, acc1)
        dot(b, 1, acc1)
        epilogue(b, 0, acc0)

        @pl.when(b == 0)
        def _():
            e_copies[2].wait()
            e_copies[3].wait()
            own_stores[1].wait()

        @pl.when(b == 1)
        def _():
            own_stores[0].wait()

        for nb in range(2, n_batch):
            @pl.when(b == nb - 1)
            def _():
                arrive(nb)

        @pl.when((b >= 1) & (b < n_batch - 1))
        def _():
            for c in loads(b + 1):
                c.start()

        @pl.when(b >= 1)
        def _():
            for c in store(b - 1, 3):
                c.start()

        for c in store(b, 0):
            c.start()
        dot(b, 2, acc0)
        epilogue(b, 1, acc1)
        dot(b, 3, acc1)
        epilogue(b, 2, acc0)
        for j in (1, 2):
            for c in store(b, j):
                c.start()
        return carry

    lax.fori_loop(0, n_batch, body, 0)
    last = n_batch - 1
    for c in store(last - 2, 3):
        c.wait()
    epilogue(last, 3, acc1)
    for c in store(last, 3):
        c.start()
    for b in range(n_batch):
        s_sum = jnp.sum(part_s[b * tiles:(b + 1) * tiles], axis=(0, 1))
        t_sum = jnp.sum(part_t[b * tiles:(b + 1) * tiles], axis=(0, 1))
        for k, row in enumerate(static_rows(b)):
            r, p = row // 512, (row // PIECE) % 4
            mine[r, p:p + 1, :] = s_sum[None, k * PIECE:(k + 1) * PIECE]
            mine[r, 4 + p:5 + p, :] = t_sum[None, k * PIECE:(k + 1) * PIECE]
    for j in range(tiles - 1):
        for c in store(last - 1, j) + store(last, j):
            c.wait()
    for c in store(last - 1, 3) + store(last, 3):
        c.wait()
    stat_copies = [pltpu.make_async_remote_copy(src_ref=mine, dst_ref=others.at[bit - 1], send_sem=stat_send.at[bit], recv_sem=stat_recv.at[bit], device_id=peer(bit), device_id_type=MESH) for bit in range(1, 8)]
    for c in stat_copies:
        c.start()
    for c in meta_copies:
        c.wait_send()
    for c in copies.values():
        c.wait_send()
    for c in stat_copies:
        c.wait()
    for r in range(8):
        t = [mine[r]] + [others[bit - 1, r ^ bit] for bit in range(1, 8)]
        stats[r] = ((t[0] + t[1]) + (t[2] + t[3])) + ((t[4] + t[5]) + (t[6] + t[7]))


def gather_logits(x_own, embed, meta_own, valid):
    rows, dim = x_own.shape
    vocab = embed.shape[0]
    toks = 8 * rows
    any_spec = pl.BlockSpec(memory_space=pl.ANY)
    vmem_spec = pl.BlockSpec(memory_space=pltpu.VMEM)
    steps = toks // 256 * (vocab // TV)
    return pl.pallas_call(
        logits_kernel,
        name="gather_logits",
        out_shape=(jax.ShapeDtypeStruct((toks, dim), jnp.bfloat16), jax.ShapeDtypeStruct((vocab, toks), jnp.float32), jax.ShapeDtypeStruct((8, 8, 128), jnp.float32), jax.ShapeDtypeStruct((8, 8, 128), jnp.int32)),
        in_specs=[any_spec, any_spec, vmem_spec, vmem_spec],
        out_specs=(any_spec, any_spec, vmem_spec, vmem_spec),
        scratch_shapes=[
            pltpu.VMEM((vocab, dim), jnp.bfloat16),
            pltpu.VMEM((2, 256, dim), jnp.bfloat16),
            pltpu.VMEM((TV, 256), jnp.float32),
            pltpu.VMEM((TV, 256), jnp.float32),
            pltpu.VMEM((2 * vocab // TV, 2, TV, PIECE), jnp.float32),
            pltpu.VMEM((steps, 8, 256), jnp.float32),
            pltpu.VMEM((steps, 8, 256), jnp.float32),
            pltpu.VMEM((8, 8, 128), jnp.float32),
            pltpu.VMEM((7, 8, 8, 128), jnp.float32),
            pltpu.SemaphoreType.DMA((vocab // TV,)),
            pltpu.SemaphoreType.DMA((4,)),
            pltpu.SemaphoreType.DMA((4 * vocab // TV,)),
            pltpu.SemaphoreType.DMA((2,)),
            pltpu.SemaphoreType.DMA((32,)),
            pltpu.SemaphoreType.DMA((32,)),
            pltpu.SemaphoreType.DMA((8,)),
            pltpu.SemaphoreType.DMA((8,)),
            pltpu.SemaphoreType.DMA((8,)),
            pltpu.SemaphoreType.DMA((8,)),
        ],
        compiler_params=pltpu.CompilerParams(collective_id=0, has_side_effects=True, vmem_limit_bytes=60 * 1024 * 1024),
        cost_estimate=pl.CostEstimate(flops=2 * toks * vocab * dim, bytes_accessed=vocab * dim * 2 + toks * vocab * 4, transcendentals=2 * toks * vocab),
    )(x_own, embed, meta_own, valid)


def part_kernel(n_add, d_log, embed, *refs):
    adds, outs = refs[:n_add], refs[n_add:]
    j = pl.program_id(0)
    half = pl.num_programs(0) // 2
    val = lax.dot_general(d_log[...], embed[...], (((0,), (0,)), ((), ())), preferred_element_type=jnp.float32)
    for c in range(2):
        @pl.when(j // half == c)
        def _():
            outs[c][...] = val + adds[c][...] if adds else val


def dx_part(d_log, embed, r, adds=()):
    vocab, dim = embed.shape
    rows, tile = 512, 512
    half = dim // tile // 2
    maps = [lambda j: (0, jnp.minimum(j, half - 1)), lambda j: (0, jnp.maximum(j - half, 0))]
    specs = [pl.BlockSpec((rows, tile), m) for m in maps]
    return pl.pallas_call(
        functools.partial(part_kernel, len(adds)),
        name="dx_part",
        grid=(2 * half,),
        out_shape=[jax.ShapeDtypeStruct((rows, dim // 2), jnp.float32)] * 2,
        in_specs=[pl.BlockSpec((vocab, rows), lambda j: (0, r)), pl.BlockSpec((vocab, tile), lambda j: (0, j))] + specs[:len(adds)],
        out_specs=specs,
        compiler_params=pltpu.CompilerParams(vmem_limit_bytes=48 * 1024 * 1024),
        cost_estimate=pl.CostEstimate(flops=2 * rows * vocab * dim, bytes_accessed=vocab * (rows + dim) * 2 + rows * dim * 4 * (1 + len(adds) // 2), transcendentals=0),
    )(d_log, embed, *adds)


def layer_norm(h_float, ln_gain, ln_bias):
    mean_val = jnp.mean(h_float, axis=-1, keepdims=True)
    centered = h_float - mean_val
    var_val = jnp.mean(centered * centered, axis=-1, keepdims=True)
    return centered * lax.rsqrt(var_val + LN_EPS) * ln_gain + ln_bias


def solution(mesh):
    def swap(bit, x):
        return lax.ppermute(x, "tp", [(i, i ^ bit) for i in range(8)])

    def group_step(hidden, ln_gain, ln_bias, out_embed, vocab_valid, targets, loss_mask):
        rows_loc, dim = hidden.shape
        vocab_loc = out_embed.shape[0]
        shard_idx = lax.axis_index("tp")
        normed, ln_back = jax.vjp(layer_norm, hidden.astype(jnp.float32), ln_gain, ln_bias)
        meta_own = jnp.concatenate([targets.reshape(4, PIECE), loss_mask.reshape(4, PIECE)])
        x_all, grad, stats, meta = gather_logits(normed.astype(jnp.bfloat16), out_embed, meta_own, (vocab_valid != 0).astype(jnp.float32)[:, None])
        sum_exp = stats[:, :4].reshape(8, rows_loc)
        tgt_tanh = stats[:, 4:].reshape(8, rows_loc)
        tgt_row = meta[:, :4].reshape(8 * rows_loc) - shard_idx * vocab_loc
        mask_all = meta[:, 4:].reshape(8, rows_loc).astype(jnp.float32)

        def group_sum(part):
            return ((part[0] + part[1]) + (part[2] + part[3])) + ((part[4] + part[5]) + (part[6] + part[7]))

        tok_count = group_sum(jnp.sum(mask_all, axis=1))
        lse = jnp.log(sum_exp)
        loss_all = (lse - SOFT_CAP * tgt_tanh + Z_COEF * lse * lse) * mask_all
        mean_loss = group_sum(jnp.sum(loss_all, axis=1)) / tok_count
        tok_coef = mask_all / tok_count
        prob_coef = ((1.0 + 2.0 * Z_COEF * lse) * tok_coef / sum_exp).reshape(1, 8 * rows_loc)
        tgt_coef = (tok_coef * (1.0 - tgt_tanh * tgt_tanh)).reshape(1, 8 * rows_loc)
        is_target = tgt_row[None, :] == jnp.arange(vocab_loc)[:, None]
        d_logits = (prob_coef * grad - jnp.where(is_target, tgt_coef, 0.0)).astype(jnp.bfloat16)
        d_logits = lax.optimization_barrier(d_logits)

        mid = dim // 2

        def part(d_log, r, c):
            rows = d_log[:, r * rows_loc:(r + 1) * rows_loc]
            return lax.dot_general(rows, out_embed[:, c * mid:(c + 1) * mid], (((0,), (0,)), ((), ())), preferred_element_type=jnp.float32)

        def after(d_log, *done):
            return lax.optimization_barrier((d_log, *done))

        far = [part(d_logits, 7, c) for c in range(2)]
        step, *far = after(d_logits, *far)
        pair_far = [part(step, 6, c) + swap(1, far[c]) for c in range(2)]
        step, *pair_far = after(step, *pair_far)
        to_x, to_y = swap(2, pair_far[0]), swap(4, pair_far[1])
        near = [*dx_part(step, out_embed, 3), *dx_part(step, out_embed, 5)]
        step, *near = after(step, *near)
        other = dx_part(step, out_embed, 1)
        got = [swap(1, x) for x in near]
        step, *other = after(step, *other)
        first_x = dx_part(step, out_embed, 2, got[:2])
        step, *first_x = after(step, *first_x)
        first_y = dx_part(step, out_embed, 4, got[2:])
        step, *first_y = after(step, *first_y)
        from_x, from_y = [swap(2, first_x[0]), None], [None, swap(4, first_y[1])]
        got = [swap(1, x) for x in other]
        own = dx_part(step, out_embed, 0, got)
        step, *own = after(step, *own)
        second = [first_x[1] + to_y, first_y[0] + to_x]
        step, *second = after(step, *second)
        from_x[1], from_y[0] = swap(2, second[0]), swap(4, second[1])
        d_embed = lax.dot_general(step, x_all, (((1,), (0,)), ((), ())), preferred_element_type=jnp.float32)
        d_normed = jnp.concatenate([own[c] + from_x[c] + from_y[c] for c in range(2)], axis=1)
        d_hidden, gain_part, bias_part = ln_back(d_normed)
        d_both = lax.psum(jnp.stack([gain_part, bias_part]), "tp")
        tok_loss = loss_all[0]
        return tok_loss, mean_loss.reshape(1), d_hidden.astype(jnp.bfloat16), d_embed, d_both[0], d_both[1]

    row_spec = P(("dp", "tp"))
    mat_spec = P(("dp", "tp"), None)

    return jax.shard_map(group_step, mesh=mesh, in_specs=(mat_spec, P(None), P(None), P("tp", None), P("tp"), row_spec, row_spec), out_specs=(row_spec, P("dp"), mat_spec, mat_spec, P("dp"), P("dp")), check_vma=False)
```

```python
import functools

import jax
import jax.numpy as jnp
from jax import lax
from jax.experimental import pallas as pl
from jax.experimental.pallas import tpu as pltpu
from jax.sharding import PartitionSpec as P


MESH = pl.DeviceIdType.MESH
SOFT_CAP = 30.0
Z_COEF = 1e-4
LN_EPS = 1e-5
PIECE = 128
TV = 1024


def batch_rows(b):
    k1 = b - 4
    k2 = b - 12
    row_a = jnp.where(b < 4, 256 * b, jnp.where(b < 12, (2 + k1 % 2) * 512 + (k1 // 2) * PIECE, (6 + k2 % 2) * 512 + (k2 // 2) * PIECE))
    row_b = jnp.where(b < 4, 256 * b + PIECE, jnp.where(b < 12, (4 + k1 % 2) * 512 + (k1 // 2) * PIECE, (6 + k2 % 2) * 512 + (2 + k2 // 2) * PIECE))
    return row_a, row_b


def static_rows(b):
    if b < 4:
        return 256 * b, 256 * b + PIECE
    if b < 12:
        k = b - 4
        return (2 + k % 2) * 512 + (k // 2) * PIECE, (4 + k % 2) * 512 + (k // 2) * PIECE
    k = b - 12
    return (6 + k % 2) * 512 + (k // 2) * PIECE, (6 + k % 2) * 512 + (2 + k // 2) * PIECE


def logits_kernel(x_own, embed, meta_own, valid, xall, grad, stats, meta, e_vmem, xbuf, acc0, acc1, out, part_s, part_t, mine, others, e_sem, x_sem, g_sem, own_sem, send_sem, recv_sem, meta_send, meta_recv, stat_send, stat_recv):
    me = lax.axis_index("tp")
    tiles = e_vmem.shape[0] // TV
    n_batch = xall.shape[0] // 256

    def peer(bit):
        return {"tp": me ^ bit}

    def fwd(src, row, bit, idx):
        return pltpu.make_async_remote_copy(src_ref=src, dst_ref=xall.at[pl.ds(row, PIECE)], send_sem=send_sem.at[idx], recv_sem=recv_sem.at[idx], device_id=peer(bit), device_id_type=MESH)

    copies = {}
    for p in range(4):
        own = x_own.at[pl.ds(p * PIECE, PIECE)]
        for r in (1, 2, 4):
            copies[r, p] = fwd(own, r * 512 + p * PIECE, r, r * 4 + p)
        copies[3, p] = fwd(xall.at[pl.ds(2 * 512 + p * PIECE, PIECE)], 3 * 512 + p * PIECE, 1, 12 + p)
        copies[5, p] = fwd(xall.at[pl.ds(4 * 512 + p * PIECE, PIECE)], 5 * 512 + p * PIECE, 1, 20 + p)
        via = (2, 4) if p < 2 else (4, 2)
        copies[6, p] = fwd(xall.at[pl.ds(via[0] * 512 + p * PIECE, PIECE)], 6 * 512 + p * PIECE, via[1], 24 + p)
        copies[7, p] = fwd(xall.at[pl.ds(6 * 512 + p * PIECE, PIECE)], 7 * 512 + p * PIECE, 1, 28 + p)

    e_copies = [pltpu.make_async_copy(embed.at[pl.ds(t * TV, TV)], e_vmem.at[pl.ds(t * TV, TV)], e_sem.at[t]) for t in range(tiles)]
    own_loads = [pltpu.make_async_copy(x_own.at[pl.ds(k * 256, 256)], xbuf.at[k], x_sem.at[2 * k]) for k in range(2)]
    own_stores = [pltpu.make_async_copy(xbuf.at[k], xall.at[pl.ds(k * 256, 256)], own_sem.at[k]) for k in range(2)]
    own_loads[0].start()
    e_copies[0].start()
    own_loads[1].start()
    for t in range(1, tiles):
        e_copies[t].start()

    barrier = pltpu.get_barrier_semaphore()
    for bit in range(1, 8):
        pl.semaphore_signal(barrier, inc=1, device_id=peer(bit), device_id_type=MESH)
    pl.semaphore_wait(barrier, 7)
    for r in (2, 4):
        copies[r, 0].start()
    for p in range(4):
        copies[1, p].start()
    meta_copies = [pltpu.make_async_remote_copy(src_ref=meta_own, dst_ref=meta.at[bit], send_sem=meta_send.at[bit], recv_sem=meta_recv.at[bit], device_id=peer(bit), device_id_type=MESH) for bit in range(1, 8)]
    for c in meta_copies:
        c.start()
    meta[0] = meta_own[...]
    own_loads[0].wait()
    own_stores[0].start()
    own_loads[1].wait()
    own_stores[1].start()

    def arrive(batch):
        if batch in (2, 4, 6):
            for r in (2, 4):
                copies[r, batch // 2].start()
        elif batch in (8, 10):
            copies[6, batch // 2 - 4].start()
        if batch in (2, 3):
            for p in range(2):
                copies[1, 2 * (batch - 2) + p].wait_recv()
        elif 4 <= batch < 12 and batch % 2 == 0:
            p = (batch - 4) // 2
            copies[4, p].wait_recv()
            if p >= 2:
                copies[6, p].start()
            copies[5, p].start()
            copies[2, p].wait_recv()
            copies[3, p].start()
        elif 4 <= batch < 12:
            p = (batch - 4) // 2
            copies[3, p].wait_recv()
            copies[5, p].wait_recv()
        elif batch % 2 == 0:
            h = (batch - 12) // 2
            for p in (h, 2 + h):
                copies[6, p].wait_recv()
                copies[7, p].start()
        else:
            h = (batch - 12) // 2
            for p in (h, 2 + h):
                copies[7, p].wait_recv()
        if batch == 2:
            for c in meta_copies:
                c.wait_recv()

    def loads(b):
        rows = batch_rows(b)
        slot = b % 2
        return [pltpu.make_async_copy(xall.at[pl.ds(pl.multiple_of(rows[k], PIECE), PIECE)], xbuf.at[slot, pl.ds(k * PIECE, PIECE)], x_sem.at[2 * slot + k]) for k in range(2)]

    row_iota = lax.broadcasted_iota(jnp.int32, (TV, 256), 0)

    def store(b, j):
        rows = batch_rows(b)
        slot = (b + 2) % 2 * tiles + j
        return [pltpu.make_async_copy(out.at[slot, k], grad.at[pl.ds(j * TV, TV), pl.ds(pl.multiple_of(rows[k], PIECE), PIECE)], g_sem.at[2 * slot + k]) for k in range(2)]

    def epilogue(b, j, acc):
        rows = batch_rows(b)
        tgt = jnp.concatenate([meta[rows[k] // 512, pl.ds((rows[k] // PIECE) % 4, 1), :] for k in range(2)], axis=1)
        ok = valid[j * TV:(j + 1) * TV, :]
        t = jnp.tanh(acc[...] * (1.0 / SOFT_CAP))
        e = jnp.exp(t * SOFT_CAP) * ok
        hit = jnp.where(row_iota == tgt - (me * (tiles * TV) + j * TV), t, 0.0)
        g = e * (1.0 - t * t)
        slot = (b + 2) % 2 * tiles + j
        for k in range(2):
            out[slot, k] = g[:, k * PIECE:(k + 1) * PIECE]
        part_s[b * tiles + j] = jnp.sum(e.reshape(TV // 8, 8, 256), axis=0)
        part_t[b * tiles + j] = jnp.sum(hit.reshape(TV // 8, 8, 256), axis=0)

    def dot(b, j, acc):
        acc[...] = lax.dot_general(e_vmem[j * TV:(j + 1) * TV, :], xbuf[b % 2], (((1,), (1,)), ((), ())), preferred_element_type=jnp.float32)

    def body(b, carry):
        before = jnp.maximum(b - 1, 0)

        @pl.when(b == 0)
        def _():
            e_copies[0].wait()
            e_copies[1].wait()

        @pl.when(b >= 2)
        def _():
            for c in loads(b):
                c.wait()

        @pl.when(b >= 3)
        def _():
            for c in store(b - 3, 3):
                c.wait()

        @pl.when(b >= 2)
        def _():
            for j in range(tiles - 1):
                for c in store(b - 2, j):
                    c.wait()

        dot(b, 0, acc0)
        epilogue(before, 3, acc1)
        dot(b, 1, acc1)
        epilogue(b, 0, acc0)

        @pl.when(b == 0)
        def _():
            e_copies[2].wait()
            e_copies[3].wait()
            own_stores[1].wait()

        @pl.when(b == 1)
        def _():
            own_stores[0].wait()

        for nb in range(2, n_batch):
            @pl.when(b == nb - 1)
            def _():
                arrive(nb)

        @pl.when((b >= 1) & (b < n_batch - 1))
        def _():
            for c in loads(b + 1):
                c.start()

        @pl.when(b >= 1)
        def _():
            for c in store(b - 1, 3):
                c.start()

        for c in store(b, 0):
            c.start()
        dot(b, 2, acc0)
        epilogue(b, 1, acc1)
        dot(b, 3, acc1)
        epilogue(b, 2, acc0)
        for j in (1, 2):
            for c in store(b, j):
                c.start()
        return carry

    lax.fori_loop(0, n_batch, body, 0)
    last = n_batch - 1
    for c in store(last - 2, 3):
        c.wait()
    epilogue(last, 3, acc1)
    for c in store(last, 3):
        c.start()
    for b in range(n_batch):
        s_sum = jnp.sum(part_s[b * tiles:(b + 1) * tiles], axis=(0, 1))
        t_sum = jnp.sum(part_t[b * tiles:(b + 1) * tiles], axis=(0, 1))
        for k, row in enumerate(static_rows(b)):
            r, p = row // 512, (row // PIECE) % 4
            mine[r, p:p + 1, :] = s_sum[None, k * PIECE:(k + 1) * PIECE]
            mine[r, 4 + p:5 + p, :] = t_sum[None, k * PIECE:(k + 1) * PIECE]
    for j in range(tiles - 1):
        for c in store(last - 1, j) + store(last, j):
            c.wait()
    for c in store(last - 1, 3) + store(last, 3):
        c.wait()
    stat_copies = [pltpu.make_async_remote_copy(src_ref=mine, dst_ref=others.at[bit - 1], send_sem=stat_send.at[bit], recv_sem=stat_recv.at[bit], device_id=peer(bit), device_id_type=MESH) for bit in range(1, 8)]
    for c in stat_copies:
        c.start()
    for c in meta_copies:
        c.wait_send()
    for c in copies.values():
        c.wait_send()
    for c in stat_copies:
        c.wait()
    for r in range(8):
        t = [mine[r]] + [others[bit - 1, r ^ bit] for bit in range(1, 8)]
        stats[r] = ((t[0] + t[1]) + (t[2] + t[3])) + ((t[4] + t[5]) + (t[6] + t[7]))


def gather_logits(x_own, embed, meta_own, valid):
    rows, dim = x_own.shape
    vocab = embed.shape[0]
    toks = 8 * rows
    any_spec = pl.BlockSpec(memory_space=pl.ANY)
    vmem_spec = pl.BlockSpec(memory_space=pltpu.VMEM)
    steps = toks // 256 * (vocab // TV)
    return pl.pallas_call(
        logits_kernel,
        name="gather_logits",
        out_shape=(jax.ShapeDtypeStruct((toks, dim), jnp.bfloat16), jax.ShapeDtypeStruct((vocab, toks), jnp.float32), jax.ShapeDtypeStruct((8, 8, 128), jnp.float32), jax.ShapeDtypeStruct((8, 8, 128), jnp.int32)),
        in_specs=[any_spec, any_spec, vmem_spec, vmem_spec],
        out_specs=(any_spec, any_spec, vmem_spec, vmem_spec),
        scratch_shapes=[
            pltpu.VMEM((vocab, dim), jnp.bfloat16),
            pltpu.VMEM((2, 256, dim), jnp.bfloat16),
            pltpu.VMEM((TV, 256), jnp.float32),
            pltpu.VMEM((TV, 256), jnp.float32),
            pltpu.VMEM((2 * vocab // TV, 2, TV, PIECE), jnp.float32),
            pltpu.VMEM((steps, 8, 256), jnp.float32),
            pltpu.VMEM((steps, 8, 256), jnp.float32),
            pltpu.VMEM((8, 8, 128), jnp.float32),
            pltpu.VMEM((7, 8, 8, 128), jnp.float32),
            pltpu.SemaphoreType.DMA((vocab // TV,)),
            pltpu.SemaphoreType.DMA((4,)),
            pltpu.SemaphoreType.DMA((4 * vocab // TV,)),
            pltpu.SemaphoreType.DMA((2,)),
            pltpu.SemaphoreType.DMA((32,)),
            pltpu.SemaphoreType.DMA((32,)),
            pltpu.SemaphoreType.DMA((8,)),
            pltpu.SemaphoreType.DMA((8,)),
            pltpu.SemaphoreType.DMA((8,)),
            pltpu.SemaphoreType.DMA((8,)),
        ],
        compiler_params=pltpu.CompilerParams(collective_id=0, has_side_effects=True, vmem_limit_bytes=60 * 1024 * 1024),
        cost_estimate=pl.CostEstimate(flops=2 * toks * vocab * dim, bytes_accessed=vocab * dim * 2 + toks * vocab * 4, transcendentals=2 * toks * vocab),
    )(x_own, embed, meta_own, valid)


def part_kernel(n_dev, n_add, *refs):
    d_logs, embed = refs[:n_dev], refs[n_dev]
    adds, outs = refs[n_dev + 1:n_dev + 1 + n_add], refs[n_dev + 1 + n_add:]
    j = pl.program_id(0)
    half = pl.num_programs(0) // 2
    vals = [lax.dot_general(d[...], embed[...], (((0,), (0,)), ((), ())), preferred_element_type=jnp.float32) for d in d_logs]
    for c in range(2):
        @pl.when(j // half == c)
        def _():
            for q, val in enumerate(vals):
                outs[2 * q + c][...] = val + adds[2 * q + c][...] if adds else val


def dx_part(d_log, embed, devs, adds=()):
    vocab, dim = embed.shape
    rows, tile = 512, 512
    half = dim // tile // 2
    maps = [lambda j: (0, jnp.minimum(j, half - 1)), lambda j: (0, jnp.maximum(j - half, 0))]
    specs = [pl.BlockSpec((rows, tile), m) for m in maps] * len(devs)
    return pl.pallas_call(
        functools.partial(part_kernel, len(devs), len(adds)),
        name="dx_part",
        grid=(2 * half,),
        out_shape=[jax.ShapeDtypeStruct((rows, dim // 2), jnp.float32)] * (2 * len(devs)),
        in_specs=[pl.BlockSpec((vocab, rows), lambda j, r=r: (0, r)) for r in devs] + [pl.BlockSpec((vocab, tile), lambda j: (0, j))] + specs[:len(adds)],
        out_specs=specs,
        compiler_params=pltpu.CompilerParams(vmem_limit_bytes=60 * 1024 * 1024),
        cost_estimate=pl.CostEstimate(flops=2 * len(devs) * rows * vocab * dim, bytes_accessed=vocab * (len(devs) * rows + dim) * 2 + len(devs) * rows * dim * 4 * (2 if adds else 1), transcendentals=0),
    )(*[d_log] * len(devs), embed, *adds)


def norm_back_kernel(own_a, own_b, x_a, x_b, y_a, y_b, hidden, gain, d_hidden, sums, acc):
    step = pl.program_id(0)
    h = hidden[...].astype(jnp.float32)
    dim = h.shape[1]
    centered = h - jnp.sum(h, axis=1, keepdims=True) * (1.0 / dim)
    rstd = lax.rsqrt(jnp.sum(centered * centered, axis=1, keepdims=True) * (1.0 / dim) + LN_EPS)
    xh = centered * rstd
    d_normed = jnp.concatenate([own_a[...] + x_a[...] + y_a[...], own_b[...] + x_b[...] + y_b[...]], axis=1)
    d_gain = d_normed * xh
    rows = h.shape[0]

    @pl.when(step == 0)
    def _():
        acc[...] = jnp.zeros_like(acc)

    acc[0] += jnp.sum(d_gain.reshape(rows // 8, 8, dim), axis=0)
    acc[1] += jnp.sum(d_normed.reshape(rows // 8, 8, dim), axis=0)
    d_xh = d_normed * gain[...]
    mean_a = jnp.sum(d_xh, axis=1, keepdims=True) * (1.0 / dim)
    mean_b = jnp.sum(d_xh * xh, axis=1, keepdims=True) * (1.0 / dim)
    d_hidden[...] = (rstd * (d_xh - mean_a - xh * mean_b)).astype(jnp.bfloat16)

    @pl.when(step == pl.num_programs(0) - 1)
    def _():
        for k in range(2):
            total = jnp.sum(acc[k], axis=0, keepdims=True)
            for q in range(4):
                sums[4 * k + q:4 * k + q + 1, :] = total[:, q * (dim // 4):(q + 1) * (dim // 4)]


def norm_back(own, from_x, from_y, hidden, ln_gain):
    rows, dim = hidden.shape
    blk = 64
    half_spec = pl.BlockSpec((blk, dim // 2), lambda i: (i, 0))
    full_spec = pl.BlockSpec((blk, dim), lambda i: (i, 0))
    return pl.pallas_call(
        norm_back_kernel,
        name="norm_back",
        grid=(rows // blk,),
        out_shape=(jax.ShapeDtypeStruct((rows, dim), jnp.bfloat16), jax.ShapeDtypeStruct((8, dim // 4), jnp.float32)),
        in_specs=[half_spec] * 6 + [full_spec, pl.BlockSpec((1, dim), lambda i: (0, 0))],
        out_specs=(full_spec, pl.BlockSpec((8, dim // 4), lambda i: (0, 0))),
        scratch_shapes=[pltpu.VMEM((2, 8, dim), jnp.float32)],
        compiler_params=pltpu.CompilerParams(vmem_limit_bytes=40 * 1024 * 1024),
        cost_estimate=pl.CostEstimate(flops=20 * rows * dim, bytes_accessed=rows * dim * 16, transcendentals=rows),
    )(*own, *from_x, *from_y, hidden, ln_gain[None, :])


def sum_kernel(mine, total, others, send_sem, recv_sem):
    me = lax.axis_index("tp")
    barrier = pltpu.get_barrier_semaphore()
    for bit in range(1, 8):
        pl.semaphore_signal(barrier, inc=1, device_id={"tp": me ^ bit}, device_id_type=MESH)
    pl.semaphore_wait(barrier, 7)
    copies = [pltpu.make_async_remote_copy(src_ref=mine, dst_ref=others.at[bit - 1], send_sem=send_sem.at[bit], recv_sem=recv_sem.at[bit], device_id={"tp": me ^ bit}, device_id_type=MESH) for bit in range(1, 8)]
    for c in copies:
        c.start()
    for c in copies:
        c.wait()
    t = [mine[...]] + [others[bit - 1] for bit in range(1, 8)]
    total[...] = ((t[0] + t[1]) + (t[2] + t[3])) + ((t[4] + t[5]) + (t[6] + t[7]))


def small_sum(x):
    vmem_spec = pl.BlockSpec(memory_space=pltpu.VMEM)
    return pl.pallas_call(
        sum_kernel,
        name="small_sum",
        out_shape=jax.ShapeDtypeStruct(x.shape, x.dtype),
        in_specs=[vmem_spec],
        out_specs=vmem_spec,
        scratch_shapes=[pltpu.VMEM((7, *x.shape), x.dtype), pltpu.SemaphoreType.DMA((8,)), pltpu.SemaphoreType.DMA((8,))],
        compiler_params=pltpu.CompilerParams(collective_id=1, has_side_effects=True),
    )(x)


def layer_norm(h_float, ln_gain, ln_bias):
    mean_val = jnp.mean(h_float, axis=-1, keepdims=True)
    centered = h_float - mean_val
    var_val = jnp.mean(centered * centered, axis=-1, keepdims=True)
    return centered * lax.rsqrt(var_val + LN_EPS) * ln_gain + ln_bias


def solution(mesh):
    def swap(bit, x):
        return lax.ppermute(x, "tp", [(i, i ^ bit) for i in range(8)])

    def group_step(hidden, ln_gain, ln_bias, out_embed, vocab_valid, targets, loss_mask):
        rows_loc, dim = hidden.shape
        vocab_loc = out_embed.shape[0]
        shard_idx = lax.axis_index("tp")
        normed = layer_norm(hidden.astype(jnp.float32), ln_gain, ln_bias)
        meta_own = jnp.concatenate([targets.reshape(4, PIECE), loss_mask.reshape(4, PIECE)])
        x_all, grad, stats, meta = gather_logits(normed.astype(jnp.bfloat16), out_embed, meta_own, (vocab_valid != 0).astype(jnp.float32)[:, None])
        sum_exp = stats[:, :4].reshape(8, rows_loc)
        tgt_tanh = stats[:, 4:].reshape(8, rows_loc)
        tgt_row = meta[:, :4].reshape(8 * rows_loc) - shard_idx * vocab_loc
        mask_all = meta[:, 4:].reshape(8, rows_loc).astype(jnp.float32)

        def group_sum(part):
            return ((part[0] + part[1]) + (part[2] + part[3])) + ((part[4] + part[5]) + (part[6] + part[7]))

        tok_count = jnp.sum(mask_all)
        lse = jnp.log(sum_exp)
        loss_all = (lse - SOFT_CAP * tgt_tanh + Z_COEF * lse * lse) * mask_all
        mean_loss = group_sum(jnp.sum(loss_all, axis=1)) / tok_count
        tok_coef = mask_all / tok_count
        prob_coef = ((1.0 + 2.0 * Z_COEF * lse) * tok_coef / sum_exp).reshape(1, 8 * rows_loc)
        tgt_coef = (tok_coef * (1.0 - tgt_tanh * tgt_tanh)).reshape(1, 8 * rows_loc)
        is_target = tgt_row[None, :] == jnp.arange(vocab_loc)[:, None]
        d_logits = (prob_coef * grad - jnp.where(is_target, tgt_coef, 0.0)).astype(jnp.bfloat16)
        d_logits = lax.optimization_barrier(d_logits)

        mid = dim // 2

        def part(d_log, r, c):
            rows = d_log[:, r * rows_loc:(r + 1) * rows_loc]
            return lax.dot_general(rows, out_embed[:, c * mid:(c + 1) * mid], (((0,), (0,)), ((), ())), preferred_element_type=jnp.float32)

        def after(d_log, *done):
            return lax.optimization_barrier((d_log, *done))

        far = [part(d_logits, 7, c) for c in range(2)]
        step, *far = after(d_logits, *far)
        pair_far = [part(step, 6, c) + swap(1, far[c]) for c in range(2)]
        step, *pair_far = after(step, *pair_far)
        to_x, to_y = swap(2, pair_far[0]), swap(4, pair_far[1])
        near = dx_part(step, out_embed, (3, 5))
        step, *near = after(step, *near)
        other = dx_part(step, out_embed, (1,))
        got = [swap(1, x) for x in near]
        step, *other = after(step, *other)
        first = dx_part(step, out_embed, (2, 4), got)
        step, *first = after(step, *first)
        first_x, first_y = first[:2], first[2:]
        from_x, from_y = [swap(2, first_x[0]), None], [None, swap(4, first_y[1])]
        got = [swap(1, x) for x in other]
        own = dx_part(step, out_embed, (0,), got)
        step, *own = after(step, *own)
        second = [first_x[1] + to_y, first_y[0] + to_x]
        step, *second = after(step, *second)
        from_x[1], from_y[0] = swap(2, second[0]), swap(4, second[1])
        d_embed = lax.dot_general(step, x_all, (((1,), (0,)), ((), ())), preferred_element_type=jnp.float32)
        d_hidden, sums = norm_back(own, from_x, from_y, hidden, ln_gain)
        d_both = small_sum(sums).reshape(2, dim)
        tok_loss = loss_all[0]
        return tok_loss, mean_loss.reshape(1), d_hidden, d_embed, d_both[0], d_both[1]

    row_spec = P(("dp", "tp"))
    mat_spec = P(("dp", "tp"), None)

    return jax.shard_map(group_step, mesh=mesh, in_specs=(mat_spec, P(None), P(None), P("tp", None), P("tp"), row_spec, row_spec), out_specs=(row_spec, P("dp"), mat_spec, mat_spec, P("dp"), P("dp")), check_vma=False)
```

```python
import functools

import jax
import jax.numpy as jnp
from jax import lax
from jax.experimental import pallas as pl
from jax.experimental.pallas import tpu as pltpu
from jax.sharding import PartitionSpec as P


MESH = pl.DeviceIdType.MESH
SOFT_CAP = 30.0
Z_COEF = 1e-4
LN_EPS = 1e-5
PIECE = 128
TV = 1024


def batch_rows(b):
    k1 = b - 4
    k2 = b - 12
    row_a = jnp.where(b < 4, 256 * b, jnp.where(b < 12, (2 + k1 % 2) * 512 + (k1 // 2) * PIECE, (6 + k2 % 2) * 512 + (k2 // 2) * PIECE))
    row_b = jnp.where(b < 4, 256 * b + PIECE, jnp.where(b < 12, (4 + k1 % 2) * 512 + (k1 // 2) * PIECE, (6 + k2 % 2) * 512 + (2 + k2 // 2) * PIECE))
    return row_a, row_b


def static_rows(b):
    if b < 4:
        return 256 * b, 256 * b + PIECE
    if b < 12:
        k = b - 4
        return (2 + k % 2) * 512 + (k // 2) * PIECE, (4 + k % 2) * 512 + (k // 2) * PIECE
    k = b - 12
    return (6 + k % 2) * 512 + (k // 2) * PIECE, (6 + k % 2) * 512 + (2 + k // 2) * PIECE


def logits_kernel(x_own, embed, meta_own, valid, xall, grad, stats, meta, e_vmem, xbuf, acc0, acc1, out, part_s, part_t, mine, others, e_sem, x_sem, g_sem, own_sem, send_sem, recv_sem, meta_send, meta_recv, stat_send, stat_recv):
    me = lax.axis_index("tp")
    tiles = e_vmem.shape[0] // TV
    n_batch = xall.shape[0] // 256

    def peer(bit):
        return {"tp": me ^ bit}

    def fwd(src, row, bit, idx):
        return pltpu.make_async_remote_copy(src_ref=src, dst_ref=xall.at[pl.ds(row, PIECE)], send_sem=send_sem.at[idx], recv_sem=recv_sem.at[idx], device_id=peer(bit), device_id_type=MESH)

    copies = {}
    for p in range(4):
        own = x_own.at[pl.ds(p * PIECE, PIECE)]
        for r in (1, 2, 4):
            copies[r, p] = fwd(own, r * 512 + p * PIECE, r, r * 4 + p)
        copies[3, p] = fwd(xall.at[pl.ds(2 * 512 + p * PIECE, PIECE)], 3 * 512 + p * PIECE, 1, 12 + p)
        copies[5, p] = fwd(xall.at[pl.ds(4 * 512 + p * PIECE, PIECE)], 5 * 512 + p * PIECE, 1, 20 + p)
        via = (2, 4) if p < 2 else (4, 2)
        copies[6, p] = fwd(xall.at[pl.ds(via[0] * 512 + p * PIECE, PIECE)], 6 * 512 + p * PIECE, via[1], 24 + p)
        copies[7, p] = fwd(xall.at[pl.ds(6 * 512 + p * PIECE, PIECE)], 7 * 512 + p * PIECE, 1, 28 + p)

    e_copies = [pltpu.make_async_copy(embed.at[pl.ds(t * TV, TV)], e_vmem.at[pl.ds(t * TV, TV)], e_sem.at[t]) for t in range(tiles)]
    own_loads = [pltpu.make_async_copy(x_own.at[pl.ds(k * 256, 256)], xbuf.at[k], x_sem.at[2 * k]) for k in range(2)]
    own_stores = [pltpu.make_async_copy(xbuf.at[k], xall.at[pl.ds(k * 256, 256)], own_sem.at[k]) for k in range(2)]
    own_loads[0].start()
    e_copies[0].start()
    own_loads[1].start()
    for t in range(1, tiles):
        e_copies[t].start()

    barrier = pltpu.get_barrier_semaphore()
    for bit in range(1, 8):
        pl.semaphore_signal(barrier, inc=1, device_id=peer(bit), device_id_type=MESH)
    pl.semaphore_wait(barrier, 7)
    for r in (2, 4):
        copies[r, 0].start()
    for p in range(4):
        copies[1, p].start()
    meta_copies = [pltpu.make_async_remote_copy(src_ref=meta_own, dst_ref=meta.at[bit], send_sem=meta_send.at[bit], recv_sem=meta_recv.at[bit], device_id=peer(bit), device_id_type=MESH) for bit in range(1, 8)]
    for c in meta_copies:
        c.start()
    meta[0] = meta_own[...]
    own_loads[0].wait()
    own_stores[0].start()
    own_loads[1].wait()
    own_stores[1].start()

    def arrive(batch):
        if batch in (2, 4, 6):
            for r in (2, 4):
                copies[r, batch // 2].start()
        elif batch in (8, 10):
            copies[6, batch // 2 - 4].start()
        if batch in (2, 3):
            for p in range(2):
                copies[1, 2 * (batch - 2) + p].wait_recv()
        elif 4 <= batch < 12 and batch % 2 == 0:
            p = (batch - 4) // 2
            copies[4, p].wait_recv()
            if p >= 2:
                copies[6, p].start()
            copies[5, p].start()
            copies[2, p].wait_recv()
            copies[3, p].start()
        elif 4 <= batch < 12:
            p = (batch - 4) // 2
            copies[3, p].wait_recv()
            copies[5, p].wait_recv()
        elif batch % 2 == 0:
            h = (batch - 12) // 2
            for p in (h, 2 + h):
                copies[6, p].wait_recv()
                copies[7, p].start()
        else:
            h = (batch - 12) // 2
            for p in (h, 2 + h):
                copies[7, p].wait_recv()
        if batch == 2:
            for c in meta_copies:
                c.wait_recv()

    def loads(b):
        rows = batch_rows(b)
        slot = b % 2
        return [pltpu.make_async_copy(xall.at[pl.ds(pl.multiple_of(rows[k], PIECE), PIECE)], xbuf.at[slot, pl.ds(k * PIECE, PIECE)], x_sem.at[2 * slot + k]) for k in range(2)]

    row_iota = lax.broadcasted_iota(jnp.int32, (TV, 256), 0)

    def store(b, j):
        rows = batch_rows(b)
        slot = (b + 2) % 2 * tiles + j
        return [pltpu.make_async_copy(out.at[slot, k], grad.at[pl.ds(j * TV, TV), pl.ds(pl.multiple_of(rows[k], PIECE), PIECE)], g_sem.at[2 * slot + k]) for k in range(2)]

    def epilogue(b, j, acc):
        rows = batch_rows(b)
        tgt = jnp.concatenate([meta[rows[k] // 512, pl.ds((rows[k] // PIECE) % 4, 1), :] for k in range(2)], axis=1)
        ok = valid[j * TV:(j + 1) * TV, :]
        t = jnp.tanh(acc[...] * (1.0 / SOFT_CAP))
        e = jnp.exp(t * SOFT_CAP) * ok
        hit = jnp.where(row_iota == tgt - (me * (tiles * TV) + j * TV), t, 0.0)
        g = e * (1.0 - t * t)
        slot = (b + 2) % 2 * tiles + j
        for k in range(2):
            out[slot, k] = g[:, k * PIECE:(k + 1) * PIECE]
        part_s[b * tiles + j] = jnp.sum(e.reshape(TV // 8, 8, 256), axis=0)
        part_t[b * tiles + j] = jnp.sum(hit.reshape(TV // 8, 8, 256), axis=0)

    def dot(b, j, acc):
        acc[...] = lax.dot_general(e_vmem[j * TV:(j + 1) * TV, :], xbuf[b % 2], (((1,), (1,)), ((), ())), preferred_element_type=jnp.float32)

    def body(b, carry):
        before = jnp.maximum(b - 1, 0)

        @pl.when(b == 0)
        def _():
            e_copies[0].wait()
            e_copies[1].wait()

        @pl.when(b >= 2)
        def _():
            for c in loads(b):
                c.wait()

        @pl.when(b >= 3)
        def _():
            for c in store(b - 3, 3):
                c.wait()

        @pl.when(b >= 2)
        def _():
            for j in range(tiles - 1):
                for c in store(b - 2, j):
                    c.wait()

        dot(b, 0, acc0)
        epilogue(before, 3, acc1)
        dot(b, 1, acc1)
        epilogue(b, 0, acc0)

        @pl.when(b == 0)
        def _():
            e_copies[2].wait()
            e_copies[3].wait()
            own_stores[1].wait()

        @pl.when(b == 1)
        def _():
            own_stores[0].wait()

        for nb in range(2, n_batch):
            @pl.when(b == nb - 1)
            def _():
                arrive(nb)

        @pl.when((b >= 1) & (b < n_batch - 1))
        def _():
            for c in loads(b + 1):
                c.start()

        @pl.when(b >= 1)
        def _():
            for c in store(b - 1, 3):
                c.start()

        for c in store(b, 0):
            c.start()
        dot(b, 2, acc0)
        epilogue(b, 1, acc1)
        dot(b, 3, acc1)
        epilogue(b, 2, acc0)
        for j in (1, 2):
            for c in store(b, j):
                c.start()
        return carry

    lax.fori_loop(0, n_batch, body, 0)
    last = n_batch - 1
    for c in store(last - 2, 3):
        c.wait()
    epilogue(last, 3, acc1)
    for c in store(last, 3):
        c.start()
    for b in range(n_batch):
        s_sum = jnp.sum(part_s[b * tiles:(b + 1) * tiles], axis=(0, 1))
        t_sum = jnp.sum(part_t[b * tiles:(b + 1) * tiles], axis=(0, 1))
        for k, row in enumerate(static_rows(b)):
            r, p = row // 512, (row // PIECE) % 4
            mine[r, p:p + 1, :] = s_sum[None, k * PIECE:(k + 1) * PIECE]
            mine[r, 4 + p:5 + p, :] = t_sum[None, k * PIECE:(k + 1) * PIECE]
    for j in range(tiles - 1):
        for c in store(last - 1, j) + store(last, j):
            c.wait()
    for c in store(last - 1, 3) + store(last, 3):
        c.wait()
    stat_copies = [pltpu.make_async_remote_copy(src_ref=mine, dst_ref=others.at[bit - 1], send_sem=stat_send.at[bit], recv_sem=stat_recv.at[bit], device_id=peer(bit), device_id_type=MESH) for bit in range(1, 8)]
    for c in stat_copies:
        c.start()
    for c in meta_copies:
        c.wait_send()
    for c in copies.values():
        c.wait_send()
    for c in stat_copies:
        c.wait()
    for r in range(8):
        t = [mine[r]] + [others[bit - 1, r ^ bit] for bit in range(1, 8)]
        stats[r] = ((t[0] + t[1]) + (t[2] + t[3])) + ((t[4] + t[5]) + (t[6] + t[7]))


def gather_logits(x_own, embed, meta_own, valid):
    rows, dim = x_own.shape
    vocab = embed.shape[0]
    toks = 8 * rows
    any_spec = pl.BlockSpec(memory_space=pl.ANY)
    vmem_spec = pl.BlockSpec(memory_space=pltpu.VMEM)
    steps = toks // 256 * (vocab // TV)
    return pl.pallas_call(
        logits_kernel,
        name="gather_logits",
        out_shape=(jax.ShapeDtypeStruct((toks, dim), jnp.bfloat16), jax.ShapeDtypeStruct((vocab, toks), jnp.float32), jax.ShapeDtypeStruct((8, 8, 128), jnp.float32), jax.ShapeDtypeStruct((8, 8, 128), jnp.int32)),
        in_specs=[any_spec, any_spec, vmem_spec, vmem_spec],
        out_specs=(any_spec, any_spec, vmem_spec, vmem_spec),
        scratch_shapes=[
            pltpu.VMEM((vocab, dim), jnp.bfloat16),
            pltpu.VMEM((2, 256, dim), jnp.bfloat16),
            pltpu.VMEM((TV, 256), jnp.float32),
            pltpu.VMEM((TV, 256), jnp.float32),
            pltpu.VMEM((2 * vocab // TV, 2, TV, PIECE), jnp.float32),
            pltpu.VMEM((steps, 8, 256), jnp.float32),
            pltpu.VMEM((steps, 8, 256), jnp.float32),
            pltpu.VMEM((8, 8, 128), jnp.float32),
            pltpu.VMEM((7, 8, 8, 128), jnp.float32),
            pltpu.SemaphoreType.DMA((vocab // TV,)),
            pltpu.SemaphoreType.DMA((4,)),
            pltpu.SemaphoreType.DMA((4 * vocab // TV,)),
            pltpu.SemaphoreType.DMA((2,)),
            pltpu.SemaphoreType.DMA((32,)),
            pltpu.SemaphoreType.DMA((32,)),
            pltpu.SemaphoreType.DMA((8,)),
            pltpu.SemaphoreType.DMA((8,)),
            pltpu.SemaphoreType.DMA((8,)),
            pltpu.SemaphoreType.DMA((8,)),
        ],
        compiler_params=pltpu.CompilerParams(collective_id=0, has_side_effects=True, vmem_limit_bytes=60 * 1024 * 1024),
        cost_estimate=pl.CostEstimate(flops=2 * toks * vocab * dim, bytes_accessed=vocab * dim * 2 + toks * vocab * 4, transcendentals=2 * toks * vocab),
    )(x_own, embed, meta_own, valid)


def part_kernel(n_dev, n_add, *refs):
    d_logs, embed = refs[:n_dev], refs[n_dev]
    adds, outs = refs[n_dev + 1:n_dev + 1 + n_add], refs[n_dev + 1 + n_add:]
    j = pl.program_id(0)
    half = pl.num_programs(0) // 2
    vals = [lax.dot_general(d[...], embed[...], (((0,), (0,)), ((), ())), preferred_element_type=jnp.float32) for d in d_logs]
    for c in range(2):
        @pl.when(j // half == c)
        def _():
            for q, val in enumerate(vals):
                outs[2 * q + c][...] = val + adds[2 * q + c][...] if adds else val


def dx_part(d_log, embed, devs, adds=()):
    vocab, dim = embed.shape
    rows, tile = 512, 512
    half = dim // tile // 2
    maps = [lambda j: (0, jnp.minimum(j, half - 1)), lambda j: (0, jnp.maximum(j - half, 0))]
    specs = [pl.BlockSpec((rows, tile), m) for m in maps] * len(devs)
    return pl.pallas_call(
        functools.partial(part_kernel, len(devs), len(adds)),
        name="dx_part",
        grid=(2 * half,),
        out_shape=[jax.ShapeDtypeStruct((rows, dim // 2), jnp.float32)] * (2 * len(devs)),
        in_specs=[pl.BlockSpec((vocab, rows), lambda j, r=r: (0, r)) for r in devs] + [pl.BlockSpec((vocab, tile), lambda j: (0, j))] + specs[:len(adds)],
        out_specs=specs,
        compiler_params=pltpu.CompilerParams(vmem_limit_bytes=60 * 1024 * 1024),
        cost_estimate=pl.CostEstimate(flops=2 * len(devs) * rows * vocab * dim, bytes_accessed=vocab * (len(devs) * rows + dim) * 2 + len(devs) * rows * dim * 4 * (2 if adds else 1), transcendentals=0),
    )(*[d_log] * len(devs), embed, *adds)


def norm_back_kernel(own_a, own_b, x_a, x_b, y_a, y_b, hidden, gain, d_hidden, sums, acc):
    step = pl.program_id(0)
    h = hidden[...].astype(jnp.float32)
    dim = h.shape[1]
    centered = h - jnp.sum(h, axis=1, keepdims=True) * (1.0 / dim)
    rstd = lax.rsqrt(jnp.sum(centered * centered, axis=1, keepdims=True) * (1.0 / dim) + LN_EPS)
    xh = centered * rstd
    d_normed = jnp.concatenate([own_a[...] + x_a[...] + y_a[...], own_b[...] + x_b[...] + y_b[...]], axis=1)
    d_gain = d_normed * xh
    rows = h.shape[0]

    @pl.when(step == 0)
    def _():
        acc[...] = jnp.zeros_like(acc)

    acc[0] += jnp.sum(d_gain.reshape(rows // 8, 8, dim), axis=0)
    acc[1] += jnp.sum(d_normed.reshape(rows // 8, 8, dim), axis=0)
    d_xh = d_normed * gain[...]
    mean_a = jnp.sum(d_xh, axis=1, keepdims=True) * (1.0 / dim)
    mean_b = jnp.sum(d_xh * xh, axis=1, keepdims=True) * (1.0 / dim)
    d_hidden[...] = (rstd * (d_xh - mean_a - xh * mean_b)).astype(jnp.bfloat16)

    @pl.when(step == pl.num_programs(0) - 1)
    def _():
        for k in range(2):
            total = jnp.sum(acc[k], axis=0, keepdims=True)
            for q in range(4):
                sums[4 * k + q:4 * k + q + 1, :] = total[:, q * (dim // 4):(q + 1) * (dim // 4)]


def norm_back(own, from_x, from_y, hidden, ln_gain):
    rows, dim = hidden.shape
    blk = 64
    half_spec = pl.BlockSpec((blk, dim // 2), lambda i: (i, 0))
    full_spec = pl.BlockSpec((blk, dim), lambda i: (i, 0))
    return pl.pallas_call(
        norm_back_kernel,
        name="norm_back",
        grid=(rows // blk,),
        out_shape=(jax.ShapeDtypeStruct((rows, dim), jnp.bfloat16), jax.ShapeDtypeStruct((8, dim // 4), jnp.float32)),
        in_specs=[half_spec] * 6 + [full_spec, pl.BlockSpec((1, dim), lambda i: (0, 0))],
        out_specs=(full_spec, pl.BlockSpec((8, dim // 4), lambda i: (0, 0))),
        scratch_shapes=[pltpu.VMEM((2, 8, dim), jnp.float32)],
        compiler_params=pltpu.CompilerParams(vmem_limit_bytes=40 * 1024 * 1024),
        cost_estimate=pl.CostEstimate(flops=20 * rows * dim, bytes_accessed=rows * dim * 16, transcendentals=rows),
    )(*own, *from_x, *from_y, hidden, ln_gain[None, :])


def sum_kernel(mine, total, others, send_sem, recv_sem):
    me = lax.axis_index("tp")
    barrier = pltpu.get_barrier_semaphore()
    for bit in range(1, 8):
        pl.semaphore_signal(barrier, inc=1, device_id={"tp": me ^ bit}, device_id_type=MESH)
    pl.semaphore_wait(barrier, 7)
    copies = [pltpu.make_async_remote_copy(src_ref=mine, dst_ref=others.at[bit - 1], send_sem=send_sem.at[bit], recv_sem=recv_sem.at[bit], device_id={"tp": me ^ bit}, device_id_type=MESH) for bit in range(1, 8)]
    for c in copies:
        c.start()
    for c in copies:
        c.wait()
    t = [mine[...]] + [others[bit - 1] for bit in range(1, 8)]
    total[...] = ((t[0] + t[1]) + (t[2] + t[3])) + ((t[4] + t[5]) + (t[6] + t[7]))


def small_sum(x):
    vmem_spec = pl.BlockSpec(memory_space=pltpu.VMEM)
    return pl.pallas_call(
        sum_kernel,
        name="small_sum",
        out_shape=jax.ShapeDtypeStruct(x.shape, x.dtype),
        in_specs=[vmem_spec],
        out_specs=vmem_spec,
        scratch_shapes=[pltpu.VMEM((7, *x.shape), x.dtype), pltpu.SemaphoreType.DMA((8,)), pltpu.SemaphoreType.DMA((8,))],
        compiler_params=pltpu.CompilerParams(collective_id=1, has_side_effects=True),
    )(x)


def norm_kernel(hidden, gain, bias, x):
    h = hidden[...].astype(jnp.float32)
    dim = h.shape[1]
    centered = h - jnp.sum(h, axis=1, keepdims=True) * (1.0 / dim)
    rstd = lax.rsqrt(jnp.sum(centered * centered, axis=1, keepdims=True) * (1.0 / dim) + LN_EPS)
    x[...] = (centered * rstd * gain[...] + bias[...]).astype(jnp.bfloat16)


def norm_forward(hidden, ln_gain, ln_bias):
    rows, dim = hidden.shape
    blk = 64
    full_spec = pl.BlockSpec((blk, dim), lambda i: (i, 0))
    row_spec = pl.BlockSpec((1, dim), lambda i: (0, 0))
    return pl.pallas_call(
        norm_kernel,
        name="norm_forward",
        grid=(rows // blk,),
        out_shape=jax.ShapeDtypeStruct((rows, dim), jnp.bfloat16),
        in_specs=[full_spec, row_spec, row_spec],
        out_specs=full_spec,
        compiler_params=pltpu.CompilerParams(vmem_limit_bytes=32 * 1024 * 1024),
        cost_estimate=pl.CostEstimate(flops=8 * rows * dim, bytes_accessed=rows * dim * 4, transcendentals=rows),
    )(hidden, ln_gain[None, :], ln_bias[None, :])


def solution(mesh):
    def swap(bit, x):
        return lax.ppermute(x, "tp", [(i, i ^ bit) for i in range(8)])

    def group_step(hidden, ln_gain, ln_bias, out_embed, vocab_valid, targets, loss_mask):
        rows_loc, dim = hidden.shape
        vocab_loc = out_embed.shape[0]
        shard_idx = lax.axis_index("tp")
        normed = norm_forward(hidden, ln_gain, ln_bias)
        meta_own = jnp.concatenate([targets.reshape(4, PIECE), loss_mask.reshape(4, PIECE)])
        x_all, grad, stats, meta = gather_logits(normed, out_embed, meta_own, (vocab_valid != 0).astype(jnp.float32)[:, None])
        sum_exp = stats[:, :4].reshape(8, rows_loc)
        tgt_tanh = stats[:, 4:].reshape(8, rows_loc)
        tgt_row = meta[:, :4].reshape(8 * rows_loc) - shard_idx * vocab_loc
        mask_all = meta[:, 4:].reshape(8, rows_loc).astype(jnp.float32)

        def group_sum(part):
            return ((part[0] + part[1]) + (part[2] + part[3])) + ((part[4] + part[5]) + (part[6] + part[7]))

        tok_count = jnp.sum(mask_all)
        lse = jnp.log(sum_exp)
        loss_all = (lse - SOFT_CAP * tgt_tanh + Z_COEF * lse * lse) * mask_all
        mean_loss = group_sum(jnp.sum(loss_all, axis=1)) / tok_count
        tok_coef = mask_all / tok_count
        prob_coef = ((1.0 + 2.0 * Z_COEF * lse) * tok_coef / sum_exp).reshape(1, 8 * rows_loc)
        tgt_coef = (tok_coef * (1.0 - tgt_tanh * tgt_tanh)).reshape(1, 8 * rows_loc)
        is_target = tgt_row[None, :] == jnp.arange(vocab_loc)[:, None]
        d_logits = (prob_coef * grad - jnp.where(is_target, tgt_coef, 0.0)).astype(jnp.bfloat16)
        d_logits = lax.optimization_barrier(d_logits)

        mid = dim // 2

        def part(d_log, r, c):
            rows = d_log[:, r * rows_loc:(r + 1) * rows_loc]
            return lax.dot_general(rows, out_embed[:, c * mid:(c + 1) * mid], (((0,), (0,)), ((), ())), preferred_element_type=jnp.float32)

        def after(d_log, *done):
            return lax.optimization_barrier((d_log, *done))

        far = [part(d_logits, 7, c) for c in range(2)]
        step, *far = after(d_logits, *far)
        pair_far = [part(step, 6, c) + swap(1, far[c]) for c in range(2)]
        step, *pair_far = after(step, *pair_far)
        to_x, to_y = swap(2, pair_far[0]), swap(4, pair_far[1])
        near = dx_part(step, out_embed, (3, 5))
        step, *near = after(step, *near)
        other = dx_part(step, out_embed, (1,))
        got = [swap(1, x) for x in near]
        step, *other = after(step, *other)
        first = dx_part(step, out_embed, (2, 4), got)
        step, *first = after(step, *first)
        first_x, first_y = first[:2], first[2:]
        from_x, from_y = [swap(2, first_x[0]), None], [None, swap(4, first_y[1])]
        got = [swap(1, x) for x in other]
        own = dx_part(step, out_embed, (0,), got)
        step, *own = after(step, *own)
        second = [first_x[1] + to_y, first_y[0] + to_x]
        step, *second = after(step, *second)
        from_x[1], from_y[0] = swap(2, second[0]), swap(4, second[1])
        d_embed = lax.dot_general(step, x_all, (((1,), (0,)), ((), ())), preferred_element_type=jnp.float32)
        d_hidden, sums = norm_back(own, from_x, from_y, hidden, ln_gain)
        d_both = small_sum(sums).reshape(2, dim)
        tok_loss = loss_all[0]
        return tok_loss, mean_loss.reshape(1), d_hidden, d_embed, d_both[0], d_both[1]

    row_spec = P(("dp", "tp"))
    mat_spec = P(("dp", "tp"), None)

    return jax.shard_map(group_step, mesh=mesh, in_specs=(mat_spec, P(None), P(None), P("tp", None), P("tp"), row_spec, row_spec), out_specs=(row_spec, P("dp"), mat_spec, mat_spec, P("dp"), P("dp")), check_vma=False)
```
